8 devices in a mesh: dp: 1 (over z), tp: 8 (over y, x, core).
Axes of the slice: x: 2, y: 2, z: 1, core: 2. Of those that a mesh axis runs over, the one named last changes fastest.
Arguments:
- hidden: bfloat16 [128, 1, 1536], P('dp')
- ln_gain: bfloat16 [2, 2, 1536], replicated
- ln_shift: bfloat16 [2, 2, 1536], replicated
- w_qkv: bfloat16 [2, 1536, 4608], P(None, None, 'tp')
- b_qkv: bfloat16 [2, 4608], P(None, 'tp')
- w_out: bfloat16 [2, 1536, 1536], P(None, 'tp')
- b_out: bfloat16 [2, 1536], replicated
- w_up: bfloat16 [2, 1536, 6144], P(None, None, 'tp')
- b_up: bfloat16 [2, 6144], P(None, 'tp')
- w_down: bfloat16 [2, 6144, 1536], P(None, 'tp')
- b_down: bfloat16 [2, 1536], replicated
- k_cache: bfloat16 [2, 128, 256, 16, 96], P(None, 'dp', None, 'tp')
- v_cache: bfloat16 [2, 128, 256, 16, 96], P(None, 'dp', None, 'tp')
- write_slot: int32 [128], P('dp')
- key_pos: int32 [128, 256], P('dp')
- key_valid: int32 [128, 256], P('dp')
Outputs:
- output 1: bfloat16 [128, 1, 1536], P('dp')
- output 2: bfloat16 [2, 128, 256, 16, 96], P(None, 'dp', None, 'tp')
- output 3: bfloat16 [2, 128, 256, 16, 96], P(None, 'dp', None, 'tp')
All inputs are finite; a program needn't handle non-finite values.
Results may differ from the reference program's by a relative error of at most 0.0130407.
Values are sent between devices in bfloat16 or wider.
A program may use at most 1 GiB of HBM per device.

```python
import math
import jax
import jax.numpy as jnp
from jax import lax

HIDDEN = 1536
HEADS = 16
HEAD = 96
BATCH = 128
CACHE = 256
LAYERS = 2

FFN = 4 * HIDDEN
LN_EPS = 1e-5


def alibi_slopes(n_heads):
    return jnp.exp2(-8.0 * jnp.arange(1, n_heads + 1).astype(jnp.float32) / n_heads)


def layer_norm(x_rows, gain, shift):
    x_f32 = x_rows.astype(jnp.float32)
    mean_val = jnp.mean(x_f32, axis=-1, keepdims=True)
    centered = x_f32 - mean_val
    var_val = jnp.mean(centered * centered, axis=-1, keepdims=True)
    normed = centered * lax.rsqrt(var_val + LN_EPS)
    return (normed * gain.astype(jnp.float32) + shift.astype(jnp.float32)).astype(jnp.bfloat16)


def draw_normal(key, shape):
    return jax.random.normal(key, shape, jnp.float32)


def draw_layout(slot_key, pad_key):
    write_slot = jax.random.randint(slot_key, (BATCH,), 0, CACHE, dtype=jnp.int32)
    write_slot = write_slot.at[0].set(CACHE - 1)
    pad_len = jax.random.randint(pad_key, (BATCH,), 0, write_slot + 1, dtype=jnp.int32)
    pad_len = pad_len.at[0].set(0)
    t_index = jnp.arange(CACHE, dtype=jnp.int32)[None, :]
    in_row = jnp.logical_and(t_index >= pad_len[:, None], t_index <= write_slot[:, None])
    key_valid = jnp.logical_and(in_row, t_index < write_slot[:, None]).astype(jnp.int32)
    key_pos = jnp.where(in_row, t_index - pad_len[:, None], 0).astype(jnp.int32)
    return write_slot, key_pos, key_valid


def setup_inputs(seed: int = 0, part: int = 0) -> dict:
    root = jax.random.key(seed)
    wkeys = jax.random.split(root, 10)
    own_keys = jax.random.split(jax.random.fold_in(root, part), 5)
    scale_hid = HIDDEN ** -0.5
    scale_ffn = FFN ** -0.5
    write_slot, key_pos, key_valid = draw_layout(own_keys[3], own_keys[4])
    return {
        'hidden': draw_normal(own_keys[0], (BATCH, 1, HIDDEN)).astype(jnp.bfloat16),
        'ln_gain': (1.0 + 0.3 * draw_normal(wkeys[0], (LAYERS, 2, HIDDEN))).astype(jnp.bfloat16),
        'ln_shift': (0.3 * draw_normal(wkeys[1], (LAYERS, 2, HIDDEN))).astype(jnp.bfloat16),
        'w_qkv': (scale_hid * draw_normal(wkeys[2], (LAYERS, HIDDEN, 3 * HIDDEN))).astype(jnp.bfloat16),
        'b_qkv': (0.3 * draw_normal(wkeys[3], (LAYERS, 3 * HIDDEN))).astype(jnp.bfloat16),
        'w_out': (2.0 * scale_hid * draw_normal(wkeys[4], (LAYERS, HIDDEN, HIDDEN))).astype(jnp.bfloat16),
        'b_out': (0.5 * draw_normal(wkeys[5], (LAYERS, HIDDEN))).astype(jnp.bfloat16),
        'w_up': (scale_hid * draw_normal(wkeys[6], (LAYERS, HIDDEN, FFN))).astype(jnp.bfloat16),
        'b_up': (0.5 * draw_normal(wkeys[7], (LAYERS, FFN))).astype(jnp.bfloat16),
        'w_down': (scale_ffn * draw_normal(wkeys[8], (LAYERS, FFN, HIDDEN))).astype(jnp.bfloat16),
        'b_down': (0.5 * draw_normal(wkeys[9], (LAYERS, HIDDEN))).astype(jnp.bfloat16),
        'k_cache': draw_normal(own_keys[1], (LAYERS, BATCH, CACHE, HEADS, HEAD)).astype(jnp.bfloat16),
        'v_cache': draw_normal(own_keys[2], (LAYERS, BATCH, CACHE, HEADS, HEAD)).astype(jnp.bfloat16),
        'write_slot': write_slot,
        'key_pos': key_pos,
        'key_valid': key_valid,
    }


def reference(hidden, ln_gain, ln_shift, w_qkv, b_qkv, w_out, b_out, w_up, b_up, w_down, b_down, k_cache, v_cache, write_slot, key_pos, key_valid):
    slopes = alibi_slopes(HEADS)
    t_index = jnp.arange(CACHE, dtype=jnp.int32)[None, :]
    is_new = t_index == write_slot[:, None]
    allowed = jnp.logical_or(key_valid > 0, is_new)
    pos_bias = slopes[None, :, None] * key_pos.astype(jnp.float32)[:, None, :]
    pos_bias = jnp.where(allowed[:, None, :], pos_bias, -jnp.inf)
    new_mask = is_new[:, :, None, None]
    score_scale = 1.0 / math.sqrt(HEAD)

    def layer_step(x_cur, layer_args):
        gain, shift, wq_mat, bq_vec, wo_mat, bo_vec, wu_mat, bu_vec, wd_mat, bd_vec, k_old, v_old = layer_args
        normed = layer_norm(x_cur, gain[0], shift[0])
        qkv_out = (jnp.dot(normed, wq_mat, preferred_element_type=jnp.float32) + bq_vec.astype(jnp.float32)).astype(jnp.bfloat16)
        qkv_out = qkv_out.reshape(BATCH, HEADS, 3, HEAD)
        k_all = jnp.where(new_mask, qkv_out[:, None, :, 1, :], k_old)
        v_all = jnp.where(new_mask, qkv_out[:, None, :, 2, :], v_old)
        scores = jnp.einsum('bhd,bthd->bht', qkv_out[:, :, 0, :].astype(jnp.float32), k_all.astype(jnp.float32)) * score_scale + pos_bias
        attn_probs = jax.nn.softmax(scores, axis=-1).astype(jnp.bfloat16)
        attn_out = jnp.einsum('bht,bthd->bhd', attn_probs.astype(jnp.float32), v_all.astype(jnp.float32)).astype(jnp.bfloat16)
        proj_sum = jnp.dot(attn_out.reshape(BATCH, HIDDEN), wo_mat, preferred_element_type=jnp.float32)
        x_mid = (x_cur.astype(jnp.float32) + proj_sum + bo_vec.astype(jnp.float32)).astype(jnp.bfloat16)
        normed_mlp = layer_norm(x_mid, gain[1], shift[1])
        up_act = jnp.dot(normed_mlp, wu_mat, preferred_element_type=jnp.float32) + bu_vec.astype(jnp.float32)
        gelu_out = jax.nn.gelu(up_act, approximate=True).astype(jnp.bfloat16)
        down_sum = jnp.dot(gelu_out, wd_mat, preferred_element_type=jnp.float32)
        x_next = (x_mid.astype(jnp.float32) + down_sum + bd_vec.astype(jnp.float32)).astype(jnp.bfloat16)
        return x_next, (k_all, v_all)

    x_last, caches = lax.scan(layer_step, hidden[:, 0, :], (ln_gain, ln_shift, w_qkv, b_qkv, w_out, b_out, w_up, b_up, w_down, b_down, k_cache, v_cache))
    return x_last[:, None, :], caches[0], caches[1]
```

```python
import functools
import math

import jax
import jax.numpy as jnp
from jax import lax
from jax.experimental import pallas as pl
from jax.experimental.pallas import tpu as pltpu
from jax.sharding import PartitionSpec as P

MESH = pl.DeviceIdType.MESH
F32 = jnp.float32
BF16 = jnp.bfloat16
LN_EPS = 1e-5
BATCH, CACHE, HIDDEN, HEADS, HEAD, FFN = 128, 256, 1536, 16, 96, 6144
TP = 8
LOCAL_HEADS = HEADS // TP
HD = LOCAL_HEADS * HEAD
QKV = 3 * HD
FF = FFN // TP
GROUP = 8
NGROUP = BATCH // GROUP
GROWS = GROUP * LOCAL_HEADS
GK = GROUP * HD
ROWS = BATCH // TP
NCHUNK = 3
CHUNK = HIDDEN // NCHUNK
NT = (((1,), (1,)), ((), ()))


def dot(a, b):
    return jnp.dot(a, b, preferred_element_type=F32)


def dot_nt(a, b):
    return lax.dot_general(a, b, NT, preferred_element_type=F32)


def iota(shape, dim):
    return lax.broadcasted_iota(jnp.int32, shape, dim)


def one_hot(cond):
    return jnp.where(cond, 1.0, 0.0).astype(BF16)


def layer_norm(x, gain, shift):
    mean = jnp.mean(x, axis=-1, keepdims=True)
    centered = x - mean
    var = jnp.mean(centered * centered, axis=-1, keepdims=True)
    normed = centered * lax.rsqrt(var + LN_EPS)
    return (normed * gain.astype(F32) + shift.astype(F32)).astype(BF16)


def att_kernel(layer, *refs):
    if layer == 0:
        (x_ref, lng, lnb, wq_hbm, bq, wo_hbm, k_hbm, v_hbm, ws_ref, kp_ref, kv_ref,
         part_ref, k_out, v_out, bias_ref, new_ref,
         kbuf, vbuf, wq, wo, abuf, qbig, kvt, ebuf, sbuf, pbuf, ksem, vsem, wsem) = refs
    else:
        (x_ref, wq_hbm, bq, wo_hbm, k_hbm, v_hbm, bias_ref, new_ref, _, _,
         part_ref, k_out, v_out,
         kbuf, vbuf, wq, wo, abuf, qbig, kvt, ebuf, sbuf, pbuf, ksem, vsem, wsem) = refs
    wq_copy = pltpu.make_async_copy(wq_hbm.at[layer], wq, wsem.at[0])
    wq_copy.start()

    def k_in(g):
        return pltpu.make_async_copy(k_hbm.at[layer, g], kbuf.at[g], ksem.at[0, g])

    def v_in(g):
        return pltpu.make_async_copy(v_hbm.at[layer, g], vbuf.at[g], vsem.at[0, g])

    def k_back(g):
        return pltpu.make_async_copy(kbuf.at[g], k_out.at[layer, g], ksem.at[1, g])

    def v_back(g):
        return pltpu.make_async_copy(vbuf.at[g], v_out.at[layer, g], vsem.at[1, g])

    def start_in(g, c):
        k_in(g).start()
        v_in(g).start()
        return c

    lax.fori_loop(0, NGROUP, start_in, 0)
    wo_copies = [pltpu.make_async_copy(wo_hbm.at[layer], wo.at[pl.ds(i * HD, HD)], wsem.at[1 + i]) for i in range(2)]
    for copy in wo_copies:
        copy.start()

    expand = one_hot(iota((2 * BATCH, BATCH), 0) // 2 == iota((2 * BATCH, BATCH), 1))
    if layer == 0:
        def norm_rows(i, c):
            r = pl.ds(pl.multiple_of(i * 16, 16), 16)
            abuf[r, :] = layer_norm(x_ref[r, :].astype(F32), lng[0, 0:1, :], lnb[0, 0:1, :])
            return c

        lax.fori_loop(0, BATCH // 16, norm_rows, 0)
        me = lax.axis_index("tp")
        slopes = []
        for h in range(LOCAL_HEADS):
            s = jnp.float32(0.0)
            for d in range(TP):
                s = jnp.where(me == d, jnp.float32(2.0 ** (-8.0 * (LOCAL_HEADS * d + h + 1) / HEADS)), s)
            slopes.append(s)
        slope = jnp.where(iota((2 * BATCH, 1), 0) % 2 == 0, slopes[0], slopes[1])
        eye = one_hot(iota((BATCH, BATCH), 0) == iota((BATCH, BATCH), 1))
        hit = one_hot(iota((CACHE, BATCH), 0) == ws_ref[...])
        is_new = dot_nt(eye, hit)
        new_ref[...] = is_new
        allowed = one_hot(jnp.logical_or(kv_ref[...] > 0, is_new > 0.5))
        pos = dot(expand, kp_ref[...].astype(F32).astype(BF16))
        bias_ref[...] = jnp.where(dot(expand, allowed) > 0.5, slope * pos, -jnp.inf)
    else:
        abuf[...] = x_ref[...].reshape(BATCH, HIDDEN)

    wq_copy.wait()
    qkv = dot_nt(abuf[...], wq[...]) + bq[layer:layer + 1, :].astype(F32)
    qkv = qkv.astype(BF16).astype(F32)
    wide = jnp.concatenate([qkv, jnp.zeros((BATCH, 640 - QKV), F32)], axis=1)
    for i in range(5):
        t = jnp.transpose(wide[:, 128 * i:128 * (i + 1)])
        lo = 128 * i
        for h in range(LOCAL_HEADS):
            for part in range(2):
                src = h * 3 * HEAD + (part + 1) * HEAD
                dst = part * HD + h * HEAD
                a, b = max(lo, src), min(lo + 128, src + HEAD)
                if a < b:
                    kvt[dst + a - src:dst + b - src, :] = t[a - lo:b - lo, :]
    q_rows = jnp.concatenate([qkv[:, h * 3 * HEAD:h * 3 * HEAD + HEAD] for h in range(LOCAL_HEADS)], axis=1).astype(BF16)
    q_dup = dot(expand, q_rows).astype(BF16)
    col, n = iota((HD, GK), 0), iota((HD, GK), 1)
    tile = one_hot(functools.reduce(jnp.logical_or, [n == col + HD * j for j in range(GROUP)]))
    n = iota((BATCH, GK), 1)
    start = (iota((BATCH, GK), 0) % GROWS) * HEAD
    block = jnp.logical_and(n >= start, n < start + HEAD)
    for i in range(2):
        qbig[pl.ds(i * BATCH, BATCH), :] = jnp.where(block, dot(q_dup[i * BATCH:(i + 1) * BATCH], tile), 0.0).astype(BF16)

    scale = 1.0 / math.sqrt(HEAD)
    n16 = iota((GROWS, GK), 1)
    start16 = iota((GROWS, GK), 0) * HEAD
    diag = jnp.logical_and(n16 >= start16, n16 < start16 + HEAD)

    def rows16(g):
        return pl.ds(pl.multiple_of(g * GROWS, GROWS), GROWS)

    def update_and_score(g):
        k_in(g).wait()
        v_in(g).wait()
        cols = pltpu.roll(kvt[...], lax.rem(BATCH - g * GROUP, BATCH), 1)
        masks = new_ref[pl.ds(pl.multiple_of(g * GROUP, GROUP), GROUP), :]
        for j in range(GROUP):
            mask = masks[j:j + 1, :].astype(BF16) > 0
            for buf, lo in ((kbuf, 0), (vbuf, HD)):
                new = jnp.broadcast_to(cols[lo:lo + HD, j:j + 1], (HD, CACHE)).astype(BF16)
                old = buf[g, j * HD:(j + 1) * HD, :]
                buf[g, j * HD:(j + 1) * HD, :] = jnp.where(jnp.broadcast_to(mask, (HD, CACHE)), new, old)
        sbuf[rows16(g), :] = dot(qbig[rows16(g), :], kbuf[g])
        k_back(g).start()
        v_back(g).start()

    def soften(g):
        s = sbuf[rows16(g), :] * scale + bias_ref[rows16(g), :]
        e = jnp.exp(s - jnp.max(s, axis=-1, keepdims=True))
        pbuf[rows16(g), :] = (e / jnp.sum(e, axis=-1, keepdims=True)).astype(BF16)

    def mix(g):
        o = jnp.where(diag, dot_nt(pbuf[rows16(g), :], vbuf[g]), 0.0)
        w = 2 * HD
        ebuf[rows16(g), :] = sum(o[:, i * w:(i + 1) * w] for i in range(GK // w)).astype(BF16)

    def step(g, c):
        update_and_score(g)
        soften(g)
        mix(g)
        return c

    lax.fori_loop(0, NGROUP, step, 0)

    pair = one_hot(iota((BATCH, 2 * BATCH), 1) // 2 == iota((BATCH, 2 * BATCH), 0))
    o2 = dot(pair, ebuf[...]).astype(BF16)
    for copy in wo_copies:
        copy.wait()
    for c in range(NCHUNK):
        cs = slice(c * CHUNK, (c + 1) * CHUNK)
        part_ref[:, :, :, cs] = dot(o2, wo[:, cs]).reshape(4, 2, ROWS, CHUNK)

    def finish(g, c):
        k_back(g).wait()
        v_back(g).wait()
        return c

    lax.fori_loop(0, NGROUP, finish, 0)


def attention(layer, x, ln, w_qkv, b_qkv, w_out, k, v, small, prev):
    vmem, hbm = pl.BlockSpec(memory_space=pltpu.VMEM), pl.BlockSpec(memory_space=pl.ANY)
    cache = jax.ShapeDtypeStruct(k.shape, BF16)
    part = jax.ShapeDtypeStruct((4, 2, ROWS, HIDDEN), F32)
    if layer == 0:
        args = (x, *ln, w_qkv, b_qkv, w_out, k, v, *small)
        in_specs = [vmem, vmem, vmem, hbm, vmem, hbm, hbm, hbm, vmem, vmem, vmem]
        outs = (part, cache, cache, jax.ShapeDtypeStruct((2 * BATCH, CACHE), F32), jax.ShapeDtypeStruct((BATCH, CACHE), F32))
        out_specs = (vmem, hbm, hbm, vmem, vmem)
        aliases = {}
    else:
        args = (x, w_qkv, b_qkv, w_out, k, v, *small, *prev)
        in_specs = [vmem, hbm, vmem, hbm, hbm, hbm, vmem, vmem, hbm, hbm]
        outs = (part, cache, cache)
        out_specs = (vmem, hbm, hbm)
        aliases = {8: 1, 9: 2}
    return pl.pallas_call(
        functools.partial(att_kernel, layer),
        out_shape=outs, in_specs=in_specs, out_specs=out_specs,
        input_output_aliases=aliases,
        scratch_shapes=[
            pltpu.VMEM((NGROUP, GK, CACHE), BF16),
            pltpu.VMEM((NGROUP, GK, CACHE), BF16),
            pltpu.VMEM((QKV, HIDDEN), BF16),
            pltpu.VMEM((2 * HD, HIDDEN), BF16),
            pltpu.VMEM((BATCH, HIDDEN), BF16),
            pltpu.VMEM((2 * BATCH, GK), BF16),
            pltpu.VMEM((2 * HD, BATCH), F32),
            pltpu.VMEM((2 * BATCH, 2 * HD), BF16),
            pltpu.VMEM((2 * BATCH, CACHE), F32),
            pltpu.VMEM((2 * BATCH, CACHE), BF16),
            pltpu.SemaphoreType.DMA((2, NGROUP)),
            pltpu.SemaphoreType.DMA((2, NGROUP)),
            pltpu.SemaphoreType.DMA((3,)),
        ],
        compiler_params=pltpu.CompilerParams(vmem_limit_bytes=48 * 1024 * 1024),
        cost_estimate=pl.CostEstimate(flops=400_000_000, bytes_accessed=53_000_000, transcendentals=65536),
        name=f"att{layer}",
    )(*args)


def comm_kernel(layer, part_in, x_ref, lng, lnb, bo, wu_hbm, bu, wd_hbm, bd, *refs):
    last = layer == 1
    if last:
        (x_out,) = refs[:1]
        refs = refs[1:]
    else:
        a_out, x_out = refs[:2]
        refs = refs[2:]
    (part, pair_buf, send_buf, recv_buf, own, gathered, hidden, gelu, wu, wd,
     wsem, d_send, d_recv, r_send, r_recv, g_send, g_recv) = refs
    me = lax.axis_index("tp")
    chip, core = me // 2, me % 2
    other = 1 - core
    cx, cy = chip % 2, chip // 2
    chips = [2 * (1 - cy) + (1 - cx), 2 * cy + (1 - cx), 2 * (1 - cy) + cx]
    wu_copy = pltpu.make_async_copy(wu_hbm.at[layer], wu, wsem.at[0])
    wd_copy = pltpu.make_async_copy(wd_hbm.at[layer], wd, wsem.at[1])
    wu_copy.start()
    wd_copy.start()

    barrier = pltpu.get_barrier_semaphore()
    for k in range(1, TP):
        pl.semaphore_signal(barrier, inc=1, device_id={"tp": lax.rem(me + k, TP)}, device_id_type=MESH)
    pl.semaphore_wait(barrier, TP - 1)

    def pair_copy(src, c):
        cs = pl.ds(c * CHUNK, CHUNK)
        return pltpu.make_async_remote_copy(
            src.at[:, other, :, cs], pair_buf.at[:, :, cs], d_send.at[c], d_recv.at[c],
            device_id={"tp": 2 * chip + other}, device_id_type=MESH)

    def reduce_copy(k, c):
        cs = pl.ds(c * CHUNK, CHUNK)
        return pltpu.make_async_remote_copy(
            send_buf.at[k, :, cs], recv_buf.at[k, :, cs], r_send.at[c, k], r_recv.at[c, k],
            device_id={"tp": 2 * chips[k] + core}, device_id_type=MESH)

    def gather_copy(k, c):
        cs = pl.ds(c * CHUNK, CHUNK)
        return pltpu.make_async_remote_copy(
            own.at[:, cs], gathered.at[me, :, cs], g_send.at[c, k - 1], g_recv.at[c, k - 1],
            device_id={"tp": lax.rem(me + k, TP)}, device_id_type=MESH)

    def reduce_scatter(src):
        for c in range(NCHUNK):
            cs = slice(c * CHUNK, (c + 1) * CHUNK)
            pair_copy(src, c).wait_recv()
            for k in range(3):
                send_buf[k, :, cs] = src[chips[k], core, :, cs] + pair_buf[chips[k], :, cs]
                reduce_copy(k, c).start()
        total = src[chip, core] + pair_buf[chip]
        for c in range(NCHUNK):
            for k in range(3):
                reduce_copy(k, c).wait_recv()
        for k in range(3):
            total = total + recv_buf[k]
        for c in range(NCHUNK):
            pair_copy(src, c).wait_send()
            for k in range(3):
                reduce_copy(k, c).wait_send()
        return total

    def start_gather():
        gathered[me] = own[...]
        for c in range(NCHUNK):
            for k in range(1, TP):
                gather_copy(k, c).start()

    def wait_gather(c):
        for k in range(1, TP):
            gather_copy(k, c).wait_recv()

    def end_gather():
        for c in range(NCHUNK):
            for k in range(1, TP):
                gather_copy(k, c).wait_send()

    for c in range(NCHUNK):
        pair_copy(part_in, c).start()
    total = reduce_scatter(part_in)
    if layer == 0:
        x_own = x_ref[pl.ds(pl.multiple_of(me * ROWS, ROWS), ROWS), :]
    else:
        x_own = x_ref[...]
    x_mid = (x_own.astype(F32) + total + bo[layer:layer + 1, :].astype(F32)).astype(BF16)
    own[...] = layer_norm(x_mid.astype(F32), lng[layer, 1:2, :], lnb[layer, 1:2, :])
    start_gather()
    wu_copy.wait()
    for c in range(NCHUNK):
        wait_gather(c)
        cs = slice(c * CHUNK, (c + 1) * CHUNK)
        up = dot(gathered[:, :, cs].reshape(BATCH, CHUNK), wu[cs, :])
        hidden[...] = up if c == 0 else hidden[...] + up
    act = jax.nn.gelu(hidden[...] + bu[layer:layer + 1, :].astype(F32), approximate=True)
    gelu[...] = act.astype(BF16)
    end_gather()
    wd_copy.wait()
    for c in range(NCHUNK):
        cs = slice(c * CHUNK, (c + 1) * CHUNK)
        part[:, :, :, cs] = dot(gelu[...], wd[:, cs]).reshape(4, 2, ROWS, CHUNK)
        pair_copy(part, c).start()
    total = reduce_scatter(part)
    x_new = (x_mid.astype(F32) + total + bd[layer:layer + 1, :].astype(F32)).astype(BF16)
    if last:
        own[...] = x_new
    else:
        x_out[...] = x_new
        own[...] = layer_norm(x_new.astype(F32), lng[layer + 1, 0:1, :], lnb[layer + 1, 0:1, :])
    start_gather()
    for c in range(NCHUNK):
        wait_gather(c)
    if last:
        x_out[...] = gathered[...]
    else:
        a_out[...] = gathered[...]
    end_gather()


def communicate(layer, part, x, ln, b_out, w_up, b_up, w_down, b_down):
    vmem, hbm = pl.BlockSpec(memory_space=pltpu.VMEM), pl.BlockSpec(memory_space=pl.ANY)
    full = jax.ShapeDtypeStruct((TP, ROWS, HIDDEN), BF16)
    outs = (full, jax.ShapeDtypeStruct((ROWS, HIDDEN), BF16)) if layer == 0 else (full,)
    return pl.pallas_call(
        functools.partial(comm_kernel, layer),
        out_shape=outs,
        in_specs=[vmem, vmem, vmem, vmem, vmem, hbm, vmem, hbm, vmem],
        out_specs=(vmem,) * len(outs),
        scratch_shapes=[
            pltpu.VMEM((4, 2, ROWS, HIDDEN), F32),
            pltpu.VMEM((4, ROWS, HIDDEN), F32),
            pltpu.VMEM((3, ROWS, HIDDEN), F32),
            pltpu.VMEM((3, ROWS, HIDDEN), F32),
            pltpu.VMEM((ROWS, HIDDEN), BF16),
            pltpu.VMEM((TP, ROWS, HIDDEN), BF16),
            pltpu.VMEM((BATCH, FF), F32),
            pltpu.VMEM((BATCH, FF), BF16),
            pltpu.VMEM((HIDDEN, FF), BF16),
            pltpu.VMEM((FF, HIDDEN), BF16),
            pltpu.SemaphoreType.DMA((2,)),
            pltpu.SemaphoreType.DMA((NCHUNK,)),
            pltpu.SemaphoreType.DMA((NCHUNK,)),
            pltpu.SemaphoreType.DMA((NCHUNK, 3)),
            pltpu.SemaphoreType.DMA((NCHUNK, 3)),
            pltpu.SemaphoreType.DMA((NCHUNK, TP - 1)),
            pltpu.SemaphoreType.DMA((NCHUNK, TP - 1)),
        ],
        compiler_params=pltpu.CompilerParams(collective_id=layer, has_side_effects=True, vmem_limit_bytes=24 * 1024 * 1024),
        cost_estimate=pl.CostEstimate(flops=650_000_000, bytes_accessed=6_000_000, transcendentals=98304),
        name=f"comm{layer}",
    )(part, x, *ln, b_out, w_up, b_up, w_down, b_down)


def solution(mesh):
    def device_step(hidden, ln_gain, ln_shift, w_qkv, b_qkv, w_out, b_out, w_up, b_up, w_down, b_down, k_cache, v_cache, write_slot, key_pos, key_valid):
        def stacked(cache):
            return jnp.transpose(cache, (0, 1, 3, 4, 2)).reshape(2, NGROUP, GK, CACHE)

        def unstacked(cache):
            return jnp.transpose(cache.reshape(2, BATCH, LOCAL_HEADS, HEAD, CACHE), (0, 1, 4, 2, 3))

        k, v = stacked(k_cache), stacked(v_cache)
        wq = jnp.transpose(w_qkv, (0, 2, 1))
        x = hidden[:, 0, :]
        ln = (ln_gain, ln_shift)
        small = (write_slot.reshape(1, BATCH), key_pos, key_valid)
        part, k_new, v_new, bias, is_new = attention(0, x, ln, wq, b_qkv, w_out, k, v, small, ())
        a_next, x_own = communicate(0, part, x, ln, b_out, w_up, b_up, w_down, b_down)
        part, k_new, v_new = attention(1, a_next, (), wq, b_qkv, w_out, k, v, (bias, is_new), (k_new, v_new))
        (x_last,) = communicate(1, part, x_own, ln, b_out, w_up, b_up, w_down, b_down)
        return x_last.reshape(BATCH, 1, HIDDEN), unstacked(k_new), unstacked(v_new)

    cache_spec = P(None, 'dp', None, 'tp', None)
    in_specs = (P('dp', None, None), P(), P(), P(None, None, 'tp'), P(None, 'tp'), P(None, 'tp', None), P(), P(None, None, 'tp'), P(None, 'tp'), P(None, 'tp', None), P(), cache_spec, cache_spec, P('dp'), P('dp', None), P('dp', None))
    out_specs = (P('dp', None, None), cache_spec, cache_spec)
    return jax.shard_map(device_step, mesh=mesh, in_specs=in_specs, out_specs=out_specs, check_vma=False)
```
